512 devices in a mesh: hi: 4 (over z_hi, core), mid: 4 (over x), lo: 32 (over z_lo, y).
Axes of the slice: x: 4, y: 8, z: 8 (z_hi: 2, z_lo: 4; z = z_hi * 4 + z_lo), core: 2. Of those that a mesh axis runs over, the one named last changes fastest.
Arguments:
- amplitudes: bfloat16 [16384, 16384], P('lo', ('hi', 'mid')), may hold values from -6 to 6
- hop_blocks: bfloat16 [4, 512, 512], replicated, may hold values from -1 to 2, as said below
- coupling_seed: int32 [14], replicated, may hold values from 1 to 7
Outputs:
- new_state: bfloat16 [16384, 16384], P('lo', ('hi', 'mid'))
The draws below stay inside these ranges and needn't reach their ends.
Inputs may be any that keep to these rules, and one draw needn't show every extreme that they name: hop_blocks[k, a, b] is zero where a and b differ in their number of set bits.
All inputs are finite; a program needn't handle non-finite values.
Results may differ from the reference program's by a relative error of at most 0.0064.
Values may be sent and summed in bfloat16 or wider, within the bound.
No kernel may reach another device: no remote copies, remote signals or barrier semaphores. Data moves between devices by JAX's collectives and lax.ppermute only.
A program may use at most 64 MiB of HBM per device.

```python
import math
import jax
import jax.numpy as jnp
from jax import lax

BLOCK = 512
SITES = 14
NU = 16384
ND = 16384


def draw_hop_blocks(key, part):
    noise = jnp.clip(jax.random.normal(key, (4, BLOCK, BLOCK), jnp.float32), -4.0, 4.0)
    config_ids = jnp.arange(BLOCK, dtype=jnp.int32)
    counted = jnp.zeros((BLOCK,), jnp.int32)
    for bit_pos in range(16):
        counted = counted + (config_ids >> bit_pos & 1)
    same_count = (counted[:, None] == counted[None, :]).astype(jnp.float32)
    identity = jnp.eye(BLOCK, dtype=jnp.float32)
    return (identity[None, :, :] + 0.5 * noise * same_count[None, :, :] / math.sqrt(BLOCK)).astype(jnp.bfloat16)


def with_ends(entries, stream_key, least, largest):
    longest = entries.shape.index(max(entries.shape))
    spots = []
    for shift in (0, 1):
        where = [jax.random.randint(jax.random.fold_in(stream_key, axis), (), 0, length) for axis, length in enumerate(entries.shape)]
        where[longest] = (where[longest] + shift) % entries.shape[longest]
        spots.append(tuple(where))
    return entries.at[spots[0]].set(least).at[spots[1]].set(largest)


def levels(stream_key, dims, split, least, high):
    loudness = 1.0
    for axis_at, blocks in split:
        draws = jax.random.uniform(jax.random.fold_in(jax.random.fold_in(stream_key, 6), axis_at), (blocks,), jnp.float32, least / len(split), high / len(split))
        loudness = loudness * jnp.repeat(jnp.exp(draws), dims[axis_at] // blocks).reshape((-1,) + (1,) * (len(dims) - 1 - axis_at))
    return loudness


def bell_draw(stream_key, dims, width, most, pieces=(), held_as=jnp.bfloat16):
    drawn = width * jax.random.normal(stream_key, dims, jnp.float32)
    if pieces:
        drawn = drawn * levels(stream_key, dims, pieces, -0.22, 0.18)
    return jnp.clip(drawn, -most, most).astype(held_as)


def setup_inputs(seed: int = 0) -> dict:
    key_of = jax.random.split(jax.random.key(seed), 4)
    amplitudes = bell_draw(key_of[0], (ND, NU), 1.0, 6.0, ((0, 32), (1, 16)))
    hop_blocks = draw_hop_blocks(jax.random.fold_in(key_of[3], 71), 0)
    coupling_seed = with_ends(jax.random.randint(key_of[2], (SITES,), 1, 8), jax.random.fold_in(key_of[2], 1), 1, 7).astype(jnp.int32)
    return {"amplitudes": amplitudes, "hop_blocks": hop_blocks, "coupling_seed": coupling_seed}


COUPLING = 0.06


def occupancy(indices):
    site_ids = jnp.arange(SITES, dtype=jnp.int32)
    return ((indices[:, None] >> site_ids[None, :]) & 1).astype(jnp.float32)


def diagonal_factor(up_index, down_index, coupling_seed):
    up_occupied = occupancy(up_index)
    down_occupied = occupancy(down_index)
    strength = COUPLING * coupling_seed.astype(jnp.float32)
    energy = jnp.dot(up_occupied * strength[None, :], down_occupied.T, precision=lax.Precision.HIGHEST)
    return jnp.exp(-energy)


def reference(amplitudes, hop_blocks, coupling_seed):
    matrices = hop_blocks.astype(jnp.float32)
    row_block = 64
    col_block = 128
    up_index = jnp.arange(NU, dtype=jnp.int32)

    def up_section(packed):
        states, first_row = packed
        values = states.astype(jnp.float32).reshape(row_block, NU // BLOCK, BLOCK)
        first_pass = jnp.einsum("dav,wv->daw", values, matrices[0]).astype(jnp.bfloat16)
        spread = first_pass.astype(jnp.float32).reshape(row_block, BLOCK, NU // BLOCK)
        second_pass = jnp.einsum("gh,dhl->dgl", matrices[1], spread).reshape(row_block, NU)
        down_index = first_row + jnp.arange(row_block, dtype=jnp.int32)
        factor = diagonal_factor(up_index, down_index, coupling_seed).T
        return (second_pass * factor).astype(jnp.bfloat16)

    starts = jnp.arange(ND // row_block, dtype=jnp.int32) * row_block
    mixed_pass = lax.map(up_section, (amplitudes.reshape(ND // row_block, row_block, NU), starts))
    mixed_pass = mixed_pass.reshape(ND, NU)
    columns = mixed_pass.reshape(ND, NU // col_block, col_block).transpose(1, 0, 2)

    def down_section(states):
        values = states.astype(jnp.float32).reshape(ND // BLOCK, BLOCK, col_block)
        third_pass = jnp.einsum("ed,adc->aec", matrices[2], values).astype(jnp.bfloat16)
        spread = third_pass.astype(jnp.float32).reshape(BLOCK, ND // BLOCK, col_block)
        fourth_pass = jnp.einsum("gh,hrc->grc", matrices[3], spread)
        return fourth_pass.reshape(ND, col_block).astype(jnp.bfloat16)

    result = lax.map(down_section, columns)
    return result.transpose(1, 0, 2).reshape(ND, NU)
```

```python
import jax
import jax.numpy as jnp
from jax import lax
from jax.sharding import Mesh, PartitionSpec as P

BLOCK = 512
SITES = 14
COUPLING = 0.06

AXES = ("zh", "core", "x", "z1", "z0", "yh", "y0")
SIZES = (2, 2, 4, 2, 2, 4, 2)
EX1 = ("zh", "core", "x", "z1", "yh")
EX2 = ("x", "z0", "y0")
EX3 = ("yh", "y0", "zh", "z1", "z0", "core")


def exchange(value, axes):
    return lax.all_to_all(value, axes, split_axis=0, concat_axis=0, tiled=True)


def bits(index, width):
    return [(index >> (width - 1 - b)) & 1 for b in range(width)]


def interaction(coupling_seed):
    c = COUPLING * coupling_seed.astype(jnp.float32)
    zh, core, x = lax.axis_index("zh"), lax.axis_index("core"), lax.axis_index("x")
    z1, z0 = lax.axis_index("z1"), lax.axis_index("z0")
    yh, y0 = lax.axis_index("yh"), lax.axis_index("y0")
    g = jnp.arange(8, dtype=jnp.int32)
    lane = jnp.arange(128, dtype=jnp.int32)
    k = jnp.arange(BLOCK, dtype=jnp.int32)
    u_low = (zh << 4) | (core << 3) | (z1 << 2) | yh
    u = (k << 5) | u_low
    d = (
        ((g[:, None] >> 2) << 13)
        | (z0 << 12)
        | ((g[:, None] & 3) << 10)
        | (y0 << 9)
        | (x << 7)
        | lane[None, :]
    )
    sites = jnp.arange(SITES, dtype=jnp.int32)
    nu = ((u[:, None] >> sites) & 1).astype(jnp.float32)
    nd = ((d.reshape(-1)[:, None] >> sites) & 1).astype(jnp.float32)
    energy = jnp.dot(nu * c, nd.T, precision=lax.Precision.HIGHEST)
    return jnp.exp(-energy).reshape(BLOCK, 8, 128).transpose(1, 0, 2)


def step_one(amplitudes, hop):
    first = jnp.einsum(
        "dav,wv->awd", amplitudes.reshape(512, 2, 512), hop, preferred_element_type=jnp.float32
    ).astype(jnp.bfloat16)
    first = first.reshape(2, 16, 4, 2, 4, 4, 128).transpose(2, 5, 3, 4, 0, 1, 6)
    return first.reshape(128, 32, 128)


def step_two(moved, hop, factor):
    moved = moved.reshape(16, 8, 32, 128).transpose(1, 0, 2, 3).reshape(8, 512, 128)
    second = jnp.einsum("kj,gjl->gkl", hop, moved, preferred_element_type=jnp.float32)
    mixed = (second * factor).astype(jnp.bfloat16)
    mixed = mixed.reshape(8, 4, 16, 2, 4, 128).transpose(2, 0, 4, 1, 3, 5)
    return mixed.reshape(16, 8 * 4 * 8, 128)


def step_three_four(moved, hop_low, hop_high):
    data = moved.reshape(4, 1024, 128).transpose(1, 0, 2).reshape(1024, 512)
    third = jnp.einsum("nd,ed->ne", data, hop_low, preferred_element_type=jnp.float32)
    third = third.astype(jnp.bfloat16)
    third = third.reshape(2, 2, 2, 4, 4, 4, 2, 16, 32).transpose(2, 0, 3, 1, 7, 5, 6, 4, 8)
    third = third.reshape(512, 1024)
    fourth = jnp.einsum("gh,hn->gn", hop_high, third, preferred_element_type=jnp.float32)
    fourth = fourth.astype(jnp.bfloat16)
    fourth = fourth.reshape(2, 2, 4, 2, 16, 2, 2, 2, 4, 32).transpose(2, 3, 5, 0, 1, 6, 7, 4, 8, 9)
    return fourth.reshape(128, 32, 128)


def finish(moved):
    moved = moved.reshape(4, 2, 2, 2, 2, 2, 2, 16, 4, 32)
    return moved.transpose(7, 9, 4, 1, 6, 8, 2, 5, 3, 0).reshape(512, 1024)


def on_device(amplitudes, hop_blocks, coupling_seed):
    sent = exchange(step_one(amplitudes, hop_blocks[0]), EX1)
    factor = interaction(coupling_seed)
    sent = exchange(step_two(sent, hop_blocks[1], factor), EX2)
    sent = exchange(step_three_four(sent, hop_blocks[2], hop_blocks[3]), EX3)
    return finish(sent)


def solution(mesh):
    fine = Mesh(mesh.devices.reshape(SIZES), AXES)
    spec = P(("z1", "z0", "yh", "y0"), ("zh", "core", "x"))
    return jax.shard_map(
        on_device, mesh=fine, in_specs=(spec, P(), P()), out_specs=spec, check_vma=False
    )
```

```python
import jax
import jax.numpy as jnp
from jax import lax
from jax.experimental import pallas as pl
from jax.experimental.pallas import tpu as pltpu
from jax.sharding import Mesh, PartitionSpec as P

BLOCK = 512
SITES = 14
COUPLING = 0.06

AXES = ("zh", "core", "x", "z1", "z0", "yh", "y0")
SIZES = (2, 2, 4, 2, 2, 4, 2)
EX1 = ("zh", "core", "x", "z1", "yh")
EX2 = ("x", "z0", "y0")
EX3 = ("yh", "y0", "zh", "z1", "z0", "core")

NT = (((1,), (1,)), ((), ()))
NN = (((1,), (0,)), ((), ()))


def exchange(value, axes):
    return lax.all_to_all(value, axes, split_axis=0, concat_axis=0, tiled=True)


def product(left, right, dims):
    return lax.dot_general(left, right, dims, preferred_element_type=jnp.float32)


def swap_groups(parts):
    lane = lax.broadcasted_iota(jnp.int32, parts[0].shape, 1)
    low_half = lane < 64
    low_quarter = (lane & 32) == 0
    half = [None] * 4
    for j in range(2):
        low, high = parts[j], parts[j + 2]
        half[j] = jnp.where(low_half, low, pltpu.roll(high, 64, 1))
        half[j + 2] = jnp.where(low_half, pltpu.roll(low, 64, 1), high)
    out = [None] * 4
    for j in (0, 2):
        low, high = half[j], half[j + 1]
        out[j] = jnp.where(low_quarter, low, pltpu.roll(high, 32, 1))
        out[j + 1] = jnp.where(low_quarter, pltpu.roll(low, 96, 1), high)
    return out


def permuted_rows(matrix, source):
    row = lax.broadcasted_iota(jnp.int32, (BLOCK, BLOCK), 0)
    col = lax.broadcasted_iota(jnp.int32, (BLOCK, BLOCK), 1)
    pick = jnp.where(col == source(row), 1.0, 0.0).astype(jnp.bfloat16)
    return product(pick, matrix, NN).astype(jnp.bfloat16)


def first_kernel(x_ref, hop_ref, out_ref, rows_ref):
    @pl.when(pl.program_id(0) == 0)
    def _():
        rows_ref[...] = permuted_rows(hop_ref[0], lambda r: ((r & 15) << 5) | (r >> 4))

    first = product(rows_ref[...], x_ref[...], NT).astype(jnp.bfloat16)
    for x in range(4):
        out_ref[:, x] = first[:, x * 128 : (x + 1) * 128].reshape(4, 8, 16, 128)


def step_one(amplitudes, hop_blocks):
    out = pl.pallas_call(
        first_kernel,
        grid=(2,),
        in_specs=[
            pl.BlockSpec((512, 512), lambda a: (0, a)),
            pl.BlockSpec((1, 512, 512), lambda a: (0, 0, 0)),
        ],
        out_specs=pl.BlockSpec((4, 4, 8, 16, 128), lambda a: (0, 0, 0, a, 0)),
        out_shape=jax.ShapeDtypeStruct((4, 4, 8, 32, 128), jnp.bfloat16),
        scratch_shapes=[pltpu.VMEM((512, 512), jnp.bfloat16)],
        cost_estimate=pl.CostEstimate(
            flops=2 * 512 * 512 * 1536, bytes_accessed=5 << 19, transcendentals=0
        ),
        name="first",
    )(amplitudes, hop_blocks)
    return out.reshape(128, 32, 128)


def prepare_kernel(seed_ref, dev_ref, hop_ref, rows_ref, base_ref, side_ref):
    def source(r):
        return (
            ((r & 4) << 6)
            | ((r & 2) << 6)
            | ((r >> 2) & 0x78)
            | ((r & 1) << 2)
            | ((r >> 3) & 3)
        )

    rows_ref[...] = permuted_rows(hop_ref[0], source)
    cost = [COUPLING * seed_ref[i].astype(jnp.float32) for i in range(SITES)]
    place = dev_ref[0]

    def at(shift):
        return ((place >> shift) & 1).astype(jnp.float32)

    zh, core, x1, x0, z1, z0, y2, y1, y0 = [at(8 - b) for b in range(9)]
    row = lax.broadcasted_iota(jnp.int32, (BLOCK, 128), 0)
    lane = lax.broadcasted_iota(jnp.int32, (BLOCK, 128), 1)

    def bit(index, shift):
        return ((index >> shift) & 1).astype(jnp.float32)

    energy = (cost[12] * z0) * bit(row, 1) + (cost[9] * y0) * bit(row, 6)
    energy += (cost[8] * x1) * bit(row, 5) + (cost[7] * x0) * bit(row, 0)
    energy += cost[6] * (bit(row, 4) * bit(lane, 6)) + cost[5] * (bit(row, 3) * bit(lane, 5))
    for site, held in enumerate((y1, y2, z1, core, zh)):
        energy += (cost[site] * held) * bit(lane, site)
    base_ref[...] = jnp.exp(-energy)
    small = lax.broadcasted_iota(jnp.int32, (8, 128), 0)
    for g in range(8):
        for top in range(4):
            extra = bit(small, 2) * (cost[13] * float(g >> 2))
            extra += cost[11] * float(((g >> 1) & 1) * (top >> 1))
            extra += cost[10] * float((g & 1) * (top & 1))
            side_ref[g, top] = jnp.exp(-extra)


def prepare(hop_blocks, coupling_seed):
    place = lax.axis_index(AXES).astype(jnp.int32).reshape(1)
    smem = pl.BlockSpec(memory_space=pltpu.SMEM)
    return pl.pallas_call(
        prepare_kernel,
        grid=(1,),
        in_specs=[smem, smem, pl.BlockSpec((1, 512, 512), lambda i: (1, 0, 0))],
        out_specs=[
            pl.BlockSpec((512, 512), lambda i: (0, 0)),
            pl.BlockSpec((512, 128), lambda i: (0, 0)),
            pl.BlockSpec((8, 4, 8, 128), lambda i: (0, 0, 0, 0)),
        ],
        out_shape=[
            jax.ShapeDtypeStruct((512, 512), jnp.bfloat16),
            jax.ShapeDtypeStruct((512, 128), jnp.float32),
            jax.ShapeDtypeStruct((8, 4, 8, 128), jnp.float32),
        ],
        cost_estimate=pl.CostEstimate(
            flops=2 * 512 * 512 * 512, bytes_accessed=3 << 19, transcendentals=1 << 17
        ),
        name="prepare",
    )(coupling_seed, place, hop_blocks)


def second_kernel(moved_ref, rows_ref, base_ref, side_ref, out_ref):
    data = jnp.concatenate([moved_ref[:, g].reshape(512, 128) for g in range(4)], axis=1)
    second = product(rows_ref[...], data, NN)
    base = base_ref[...].reshape(4, 16, 8, 128)
    for g in range(4):
        part = second[:, g * 128 : (g + 1) * 128].reshape(4, 16, 8, 128)
        mixed = part * (base * side_ref[g][:, None])
        out_ref[:, g] = mixed.reshape(16, 32, 128).astype(jnp.bfloat16)


def step_two(moved, rows, base, side):
    out = pl.pallas_call(
        second_kernel,
        grid=(2,),
        in_specs=[
            pl.BlockSpec((16, 4, 32, 128), lambda i: (0, i, 0, 0)),
            pl.BlockSpec((512, 512), lambda i: (0, 0)),
            pl.BlockSpec((512, 128), lambda i: (0, 0)),
            pl.BlockSpec((4, 4, 8, 128), lambda i: (i, 0, 0, 0)),
        ],
        out_specs=pl.BlockSpec((16, 4, 32, 128), lambda i: (0, i, 0, 0)),
        out_shape=jax.ShapeDtypeStruct((16, 8, 32, 128), jnp.bfloat16),
        cost_estimate=pl.CostEstimate(
            flops=2 * 512 * 512 * 1024, bytes_accessed=3 << 20, transcendentals=0
        ),
        name="second",
    )(moved.reshape(16, 8, 32, 128), rows, base, side)
    return out.reshape(16, 256, 128)


def third_kernel(moved_ref, low_ref, high_ref, out_ref, held_ref):
    step = pl.program_id(0)

    @pl.when(step < 4)
    def _():
        data = jnp.concatenate([moved_ref[x, 0] for x in range(4)], axis=1)
        third = product(data, low_ref[0], NT)
        at = (step >> 1) * 128 + (step & 1) * 16
        for top in range(4):
            lanes = slice(top * 128, (top + 1) * 128)
            parts = [
                jnp.concatenate(
                    [third[(g * 4 + j) * 8 : (g * 4 + j) * 8 + 8, lanes] for g in range(8)], axis=0
                )
                for j in range(4)
            ]
            swapped = swap_groups(parts)
            for j in range(4):
                for g in range(8):
                    where = at + (g >> 2) * 256 + (g & 3) * 32 + top * 4 + j
                    held_ref[pl.ds(pl.multiple_of(where * 8, 8), 8), :] = swapped[j][
                        g * 8 : g * 8 + 8
                    ]

    @pl.when(step >= 4)
    def _():
        s = (step - 4) * 2
        data = jnp.concatenate(
            [held_ref[pl.ds(s + b, 512, stride=8), :].astype(jnp.bfloat16) for b in range(2)],
            axis=1,
        )
        fourth = product(high_ref[0], data, NN).astype(jnp.bfloat16)
        for b in range(2):
            for r in range(32):
                d13, d12, mid, d9 = r >> 4, (r >> 3) & 1, (r >> 1) & 3, r & 1
                out_ref[mid, d9, 0, d13, d12, 0, b] = fourth[
                    r * 16 : r * 16 + 16, b * 128 : (b + 1) * 128
                ]


def step_three_four(moved, hop_blocks):
    out = pl.pallas_call(
        third_kernel,
        grid=(8,),
        in_specs=[
            pl.BlockSpec((4, 1, 256, 128), lambda i: (0, jnp.minimum(i, 3), 0, 0)),
            pl.BlockSpec((1, 512, 512), lambda i: (2, 0, 0)),
            pl.BlockSpec((1, 512, 512), lambda i: (3, 0, 0)),
        ],
        out_specs=pl.BlockSpec(
            (4, 2, 1, 2, 2, 1, 2, 16, 128),
            lambda i: (
                0,
                0,
                jnp.maximum(i - 4, 0) // 2,
                0,
                0,
                jnp.maximum(i - 4, 0) % 2,
                0,
                0,
                0,
            ),
        ),
        out_shape=jax.ShapeDtypeStruct((4, 2, 2, 2, 2, 2, 2, 16, 128), jnp.bfloat16),
        scratch_shapes=[pltpu.VMEM((4096, 128), jnp.float32)],
        cost_estimate=pl.CostEstimate(
            flops=4 * 512 * 512 * 1024, bytes_accessed=3 << 20, transcendentals=0
        ),
        name="third",
    )(moved.reshape(4, 4, 256, 128), hop_blocks, hop_blocks)
    return out.reshape(128, 32, 128)


def last_kernel(moved_ref, out_ref, held_ref):
    for low in range(32):
        u4, u3, u2, u10 = low >> 4, (low >> 3) & 1, (low >> 2) & 1, low & 3
        block = moved_ref[u10, 0, u4, u2, 0, u3].astype(jnp.float32)
        for u7 in range(2):
            held_ref[(u7 * 32 + low) * 16 : (u7 * 32 + low + 1) * 16, :] = block[
                u7 * 16 : u7 * 16 + 16
            ]
    for u7 in range(2):
        for top in range(4):
            parts = [
                held_ref[pl.ds(u7 * 512 + top * 4 + j, 32, stride=16), :] for j in range(4)
            ]
            tile = jnp.concatenate(swap_groups(parts), axis=0)
            out_ref[top * 128 : (top + 1) * 128, u7 * 128 : (u7 + 1) * 128] = tile.T.astype(
                jnp.bfloat16
            )


def finish(moved):
    return pl.pallas_call(
        last_kernel,
        grid=(4,),
        in_specs=[
            pl.BlockSpec(
                (4, 1, 2, 2, 1, 2, 32, 128), lambda i: (0, i % 2, 0, 0, i // 2, 0, 0, 0)
            )
        ],
        out_specs=pl.BlockSpec((512, 256), lambda i: (0, i)),
        out_shape=jax.ShapeDtypeStruct((512, 1024), jnp.bfloat16),
        scratch_shapes=[pltpu.VMEM((1024, 128), jnp.float32)],
        name="last",
    )(moved.reshape(4, 2, 2, 2, 2, 2, 32, 128))


def on_device(amplitudes, hop_blocks, coupling_seed):
    rows, base, side = prepare(hop_blocks, coupling_seed)
    sent = exchange(step_one(amplitudes, hop_blocks), EX1)
    sent = exchange(step_two(sent, rows, base, side), EX2)
    sent = exchange(step_three_four(sent, hop_blocks), EX3)
    return finish(sent)


def solution(mesh):
    fine = Mesh(mesh.devices.reshape(SIZES), AXES)
    spec = P(("z1", "z0", "yh", "y0"), ("zh", "core", "x"))
    return jax.shard_map(
        on_device, mesh=fine, in_specs=(spec, P(), P()), out_specs=spec, check_vma=False
    )
```

```python
import jax
import jax.numpy as jnp
from jax import lax
from jax.experimental import pallas as pl
from jax.experimental.pallas import tpu as pltpu
from jax.sharding import Mesh, PartitionSpec as P

BLOCK = 512
SITES = 14
COUPLING = 0.06

AXES = ("zh", "core", "x", "z1", "z0", "yh", "y0")
SIZES = (2, 2, 4, 2, 2, 4, 2)
EX1 = ("zh", "core", "x", "z1", "yh")
EX2 = ("x", "z0", "y0")
EX3 = ("yh", "y0", "zh", "z1", "z0", "core")

NT = (((1,), (1,)), ((), ()))
NN = (((1,), (0,)), ((), ()))


def exchange(value, axes):
    return lax.all_to_all(value, axes, split_axis=0, concat_axis=0, tiled=True)


def product(left, right, dims):
    return lax.dot_general(left, right, dims, preferred_element_type=jnp.float32)


def swap_groups(parts):
    group = lax.broadcasted_iota(jnp.int32, parts[0].shape, 1) >> 5
    is_group = [group == q for q in range(3)]

    def choose(values):
        out = values[3]
        for q in range(3):
            out = jnp.where(is_group[q], values[q], out)
        return out

    turned = []
    for m in range(4):
        held = choose([parts[(q + m) & 3] for q in range(4)])
        turned.append(held if m == 0 else pltpu.roll(held, 32 * m, 1))
    return [choose([turned[(q - a) & 3] for q in range(4)]) for a in range(4)]


def permuted_rows(matrix, source):
    row = lax.broadcasted_iota(jnp.int32, (BLOCK, BLOCK), 0)
    col = lax.broadcasted_iota(jnp.int32, (BLOCK, BLOCK), 1)
    pick = jnp.where(col == source(row), 1.0, 0.0).astype(jnp.bfloat16)
    return product(pick, matrix, NN).astype(jnp.bfloat16)


def first_kernel(x_ref, hop_ref, out_ref, rows_ref):
    rows = permuted_rows(hop_ref[0], lambda r: ((r & 15) << 5) | (r >> 4))
    for u9 in range(2):
        first = product(rows, x_ref[:, u9 * 512 : (u9 + 1) * 512], NT).astype(jnp.bfloat16)
        for x in range(4):
            out_ref[:, x, :, u9 * 16 : (u9 + 1) * 16] = first[:, x * 128 : (x + 1) * 128].reshape(
                4, 8, 16, 128
            )


def step_one(amplitudes, hop_blocks):
    out = pl.pallas_call(
        first_kernel,
        grid=(1,),
        in_specs=[
            pl.BlockSpec((512, 1024), lambda i: (0, 0)),
            pl.BlockSpec((1, 512, 512), lambda i: (0, 0, 0)),
        ],
        out_specs=pl.BlockSpec((4, 4, 8, 32, 128), lambda i: (0, 0, 0, 0, 0)),
        out_shape=jax.ShapeDtypeStruct((4, 4, 8, 32, 128), jnp.bfloat16),
        scratch_shapes=[pltpu.VMEM((8, 128), jnp.float32)],
        cost_estimate=pl.CostEstimate(
            flops=2 * 512 * 512 * 1536, bytes_accessed=5 << 19, transcendentals=0
        ),
        name="first",
        compiler_params=pltpu.CompilerParams(vmem_limit_bytes=16 << 20),
    )(amplitudes, hop_blocks[:1])
    return out.reshape(128, 32, 128)


def prepare_kernel(seed_ref, dev_ref, hop_ref, rows_ref, base_ref, side_ref):
    def source(r):
        return (
            ((r & 4) << 6)
            | ((r & 2) << 6)
            | ((r >> 2) & 0x78)
            | ((r & 1) << 2)
            | ((r >> 3) & 3)
        )

    rows_ref[...] = permuted_rows(hop_ref[0], source)
    cost = [COUPLING * seed_ref[i].astype(jnp.float32) for i in range(SITES)]
    place = dev_ref[0]

    def at(shift):
        return ((place >> shift) & 1).astype(jnp.float32)

    zh, core, x1, x0, z1, z0, y2, y1, y0 = [at(8 - b) for b in range(9)]
    row = lax.broadcasted_iota(jnp.int32, (BLOCK, 128), 0)
    lane = lax.broadcasted_iota(jnp.int32, (BLOCK, 128), 1)

    def bit(index, shift):
        return ((index >> shift) & 1).astype(jnp.float32)

    energy = (cost[12] * z0) * bit(row, 1) + (cost[9] * y0) * bit(row, 6)
    energy += (cost[8] * x1) * bit(row, 5) + (cost[7] * x0) * bit(row, 0)
    energy += cost[6] * (bit(row, 4) * bit(lane, 6)) + cost[5] * (bit(row, 3) * bit(lane, 5))
    for site, held in enumerate((y1, y2, z1, core, zh)):
        energy += (cost[site] * held) * bit(lane, site)
    base_ref[...] = jnp.exp(-energy)
    small = lax.broadcasted_iota(jnp.int32, (8, 128), 0)
    for g in range(8):
        for top in range(4):
            extra = bit(small, 2) * (cost[13] * float(g >> 2))
            extra += cost[11] * float(((g >> 1) & 1) * (top >> 1))
            extra += cost[10] * float((g & 1) * (top & 1))
            side_ref[g, top] = jnp.exp(-extra)


def prepare(hop_blocks, coupling_seed):
    place = lax.axis_index(AXES).astype(jnp.int32).reshape(1)
    smem = pl.BlockSpec(memory_space=pltpu.SMEM)
    return pl.pallas_call(
        prepare_kernel,
        grid=(1,),
        in_specs=[smem, smem, pl.BlockSpec((1, 512, 512), lambda i: (1, 0, 0))],
        out_specs=[
            pl.BlockSpec((512, 512), lambda i: (0, 0)),
            pl.BlockSpec((512, 128), lambda i: (0, 0)),
            pl.BlockSpec((8, 4, 8, 128), lambda i: (0, 0, 0, 0)),
        ],
        out_shape=[
            jax.ShapeDtypeStruct((512, 512), jnp.bfloat16),
            jax.ShapeDtypeStruct((512, 128), jnp.float32),
            jax.ShapeDtypeStruct((8, 4, 8, 128), jnp.float32),
        ],
        cost_estimate=pl.CostEstimate(
            flops=2 * 512 * 512 * 512, bytes_accessed=3 << 19, transcendentals=1 << 17
        ),
        name="prepare",
        compiler_params=pltpu.CompilerParams(vmem_limit_bytes=16 << 20),
    )(coupling_seed, place, hop_blocks)


def second_kernel(moved_ref, rows_ref, base_ref, side_ref, out_ref):
    base = base_ref[...].reshape(4, 16, 8, 128)
    for half in range(4):
        data = jnp.concatenate(
            [moved_ref[:, half * 2 + g].reshape(512, 128) for g in range(2)], axis=1
        )
        second = product(rows_ref[...], data, NN)
        for b in range(2):
            g = half * 2 + b
            part = second[:, b * 128 : (b + 1) * 128].reshape(4, 16, 8, 128)
            mixed = part * (base * side_ref[g][:, None])
            out_ref[:, g] = mixed.reshape(16, 32, 128).astype(jnp.bfloat16)


def step_two(moved, rows, base, side):
    out = pl.pallas_call(
        second_kernel,
        grid=(1,),
        in_specs=[
            pl.BlockSpec((16, 8, 32, 128), lambda i: (0, i, 0, 0)),
            pl.BlockSpec((512, 512), lambda i: (0, 0)),
            pl.BlockSpec((512, 128), lambda i: (0, 0)),
            pl.BlockSpec((8, 4, 8, 128), lambda i: (i, 0, 0, 0)),
        ],
        out_specs=pl.BlockSpec((16, 8, 32, 128), lambda i: (0, i, 0, 0)),
        out_shape=jax.ShapeDtypeStruct((16, 8, 32, 128), jnp.bfloat16),
        cost_estimate=pl.CostEstimate(
            flops=2 * 512 * 512 * 1024, bytes_accessed=3 << 20, transcendentals=0
        ),
        name="second",
        compiler_params=pltpu.CompilerParams(vmem_limit_bytes=16 << 20),
    )(moved.reshape(16, 8, 32, 128), rows, base, side)
    return out.reshape(16, 256, 128)


def third_kernel(moved_ref, low_ref, high_ref, out_ref, held_ref):
    for step in range(4):
        data = jnp.concatenate([moved_ref[x, step] for x in range(4)], axis=1)
        third = product(data, low_ref[0], NT)
        at = (step >> 1) * 128 + (step & 1) * 16
        for top in range(4):
            lanes = slice(top * 128, (top + 1) * 128)
            parts = [
                jnp.concatenate(
                    [third[(g * 4 + j) * 8 : (g * 4 + j) * 8 + 8, lanes] for g in range(8)], axis=0
                )
                for j in range(4)
            ]
            swapped = swap_groups(parts)
            for j in range(4):
                for g in range(8):
                    where = (at + (g >> 2) * 256 + (g & 3) * 32 + top * 4 + j) * 8
                    held_ref[where : where + 8, :] = swapped[j][g * 8 : g * 8 + 8]
    for step in range(4):
        data = jnp.concatenate(
            [
                held_ref[pl.ds(step * 2 + b, 512, stride=8), :].astype(jnp.bfloat16)
                for b in range(2)
            ],
            axis=1,
        )
        fourth = product(high_ref[0], data, NN).astype(jnp.bfloat16)
        for b in range(2):
            for r in range(32):
                d13, d12, mid, d9 = r >> 4, (r >> 3) & 1, (r >> 1) & 3, r & 1
                out_ref[mid, d9, step >> 1, d13, d12, step & 1, b] = fourth[
                    r * 16 : r * 16 + 16, b * 128 : (b + 1) * 128
                ]


def step_three_four(moved, hop_blocks):
    out = pl.pallas_call(
        third_kernel,
        grid=(1,),
        in_specs=[
            pl.BlockSpec((4, 4, 256, 128), lambda i: (0, 0, 0, 0)),
            pl.BlockSpec((1, 512, 512), lambda i: (2, 0, 0)),
            pl.BlockSpec((1, 512, 512), lambda i: (3, 0, 0)),
        ],
        out_specs=pl.BlockSpec(
            (4, 2, 2, 2, 2, 2, 2, 16, 128), lambda i: (0, 0, 0, 0, 0, 0, 0, 0, 0)
        ),
        out_shape=jax.ShapeDtypeStruct((4, 2, 2, 2, 2, 2, 2, 16, 128), jnp.bfloat16),
        scratch_shapes=[pltpu.VMEM((4096, 128), jnp.float32)],
        cost_estimate=pl.CostEstimate(
            flops=4 * 512 * 512 * 1024, bytes_accessed=3 << 20, transcendentals=0
        ),
        name="third",
        compiler_params=pltpu.CompilerParams(vmem_limit_bytes=16 << 20),
    )(moved.reshape(4, 4, 256, 128), hop_blocks, hop_blocks)
    return out.reshape(128, 32, 128)


def last_kernel(moved_ref, out_ref, held_ref):
    row = lax.broadcasted_iota(jnp.int32, (128, 128), 0)
    col = lax.broadcasted_iota(jnp.int32, (128, 128), 1)
    eye = jnp.where(row == col, 1.0, 0.0).astype(jnp.bfloat16)
    for pair in range(2):
        u9, u8 = pair >> 1, pair & 1
        for low in range(32):
            u4, u3, u2, u10 = low >> 4, (low >> 3) & 1, (low >> 2) & 1, low & 3
            block = moved_ref[u10, u8, u4, u2, u9, u3].astype(jnp.float32)
            for u7 in range(2):
                at = ((pair * 2 + u7) * 32 + low) * 16
                held_ref[at : at + 16, :] = block[u7 * 16 : u7 * 16 + 16]
    for lane in range(4):
        for top in range(4):
            parts = [
                held_ref[pl.ds(lane * 512 + top * 4 + j, 32, stride=16), :] for j in range(4)
            ]
            tile = jnp.concatenate(swap_groups(parts), axis=0).astype(jnp.bfloat16)
            out_ref[top * 128 : (top + 1) * 128, lane * 128 : (lane + 1) * 128] = product(
                eye, tile, NT
            ).astype(jnp.bfloat16)


def finish(moved):
    return pl.pallas_call(
        last_kernel,
        grid=(2,),
        in_specs=[
            pl.BlockSpec((4, 2, 2, 2, 1, 2, 32, 128), lambda i: (0, 0, 0, 0, i, 0, 0, 0))
        ],
        out_specs=pl.BlockSpec((512, 512), lambda i: (0, i)),
        out_shape=jax.ShapeDtypeStruct((512, 1024), jnp.bfloat16),
        scratch_shapes=[pltpu.VMEM((2048, 128), jnp.float32)],
        name="last",
        compiler_params=pltpu.CompilerParams(vmem_limit_bytes=16 << 20),
    )(moved.reshape(4, 2, 2, 2, 2, 2, 32, 128))


def on_device(amplitudes, hop_blocks, coupling_seed):
    tables = prepare(hop_blocks, coupling_seed)
    sent, *tables = lax.optimization_barrier((step_one(amplitudes, hop_blocks), *tables))
    sent = exchange(sent, EX1)
    sent = exchange(step_two(sent, *tables), EX2)
    sent = exchange(step_three_four(sent, hop_blocks), EX3)
    return finish(sent)


def solution(mesh):
    fine = Mesh(mesh.devices.reshape(SIZES), AXES)
    spec = P(("z1", "z0", "yh", "y0"), ("zh", "core", "x"))
    return jax.shard_map(
        on_device, mesh=fine, in_specs=(spec, P(), P()), out_specs=spec, check_vma=False
    )
```

```python
import jax
import jax.numpy as jnp
from jax import lax
from jax.experimental import pallas as pl
from jax.experimental.pallas import tpu as pltpu
from jax.sharding import Mesh, PartitionSpec as P

BLOCK = 512
SITES = 14
COUPLING = 0.06

AXES = ("zh", "core", "x", "z1", "z0", "yh", "y0")
SIZES = (2, 2, 4, 2, 2, 4, 2)
EX1 = ("x", "yh", "zh", "z1", "core")
EX2 = ("x", "z0", "y0")
EX3 = ("yh", "y0", "zh", "z1", "z0", "core")

NT = (((1,), (1,)), ((), ()))
NN = (((1,), (0,)), ((), ()))


def exchange(value, axes):
    return lax.all_to_all(value, axes, split_axis=0, concat_axis=0, tiled=True)


def product(left, right, dims):
    return lax.dot_general(left, right, dims, preferred_element_type=jnp.float32)


def swap_groups(parts):
    group = lax.broadcasted_iota(jnp.int32, parts[0].shape, 1) >> 5
    is_group = [group == q for q in range(3)]

    def choose(values):
        out = values[3]
        for q in range(3):
            out = jnp.where(is_group[q], values[q], out)
        return out

    turned = []
    for m in range(4):
        held = choose([parts[(q + m) & 3] for q in range(4)])
        turned.append(held if m == 0 else pltpu.roll(held, 32 * m, 1))
    return [choose([turned[(q - a) & 3] for q in range(4)]) for a in range(4)]


def in_hbm(*arrays):
    return [pltpu.with_memory_space_constraint(a, pltpu.HBM) for a in arrays]


def permuted_rows(matrix, source):
    row = lax.broadcasted_iota(jnp.int32, (BLOCK, BLOCK), 0)
    col = lax.broadcasted_iota(jnp.int32, (BLOCK, BLOCK), 1)
    pick = jnp.where(col == source(row), 1.0, 0.0).astype(jnp.bfloat16)
    return product(pick, matrix, NN).astype(jnp.bfloat16)


def first_kernel(
    seed_ref, dev_ref, x_hbm, hop_hbm, out_ref, rows_ref, base_ref, side_ref, x_ref, hop_ref, sems
):
    copies = [
        pltpu.make_async_copy(hop_hbm.at[0], hop_ref.at[0], sems.at[0]),
        pltpu.make_async_copy(x_hbm.at[:, 0:512], x_ref.at[0], sems.at[1]),
        pltpu.make_async_copy(x_hbm.at[:, 512:1024], x_ref.at[1], sems.at[2]),
        pltpu.make_async_copy(hop_hbm.at[1], hop_ref.at[1], sems.at[3]),
    ]
    for copy in copies:
        copy.start()

    cost = [COUPLING * seed_ref[i].astype(jnp.float32) for i in range(SITES)]
    place = dev_ref[0]

    def at(shift):
        return ((place >> shift) & 1).astype(jnp.float32)

    zh, core, x1, x0, z1, z0, y2, y1, y0 = [at(8 - b) for b in range(9)]
    row = lax.broadcasted_iota(jnp.int32, (BLOCK, 128), 0)
    lane = lax.broadcasted_iota(jnp.int32, (BLOCK, 128), 1)

    def bit(index, shift):
        return ((index >> shift) & 1).astype(jnp.float32)

    energy = (cost[12] * z0) * bit(row, 1) + (cost[9] * y0) * bit(row, 6)
    energy += (cost[8] * x1) * bit(row, 5) + (cost[7] * x0) * bit(row, 0)
    energy += cost[6] * (bit(row, 4) * bit(lane, 6)) + cost[5] * (bit(row, 3) * bit(lane, 5))
    for site, held in enumerate((core, z1, zh, y1, y2)):
        energy += (cost[site] * held) * bit(lane, site)
    base_ref[...] = jnp.exp(-energy)
    small = lax.broadcasted_iota(jnp.int32, (8, 128), 0)
    for g in range(8):
        for top in range(4):
            extra = bit(small, 2) * (cost[13] * float(g >> 2))
            extra += cost[11] * float(((g >> 1) & 1) * (top >> 1))
            extra += cost[10] * float((g & 1) * (top & 1))
            side_ref[g, top] = jnp.exp(-extra)

    copies[0].wait()
    rows = permuted_rows(hop_ref[0], lambda r: ((r & 15) << 5) | (r >> 4))
    for u9 in range(2):
        copies[1 + u9].wait()
        first = product(rows, x_ref[u9], NT).astype(jnp.bfloat16)
        for x in range(4):
            out_ref[x, :, u9 * 16 : (u9 + 1) * 16] = first[:, x * 128 : (x + 1) * 128].reshape(
                32, 16, 128
            )

    def source(r):
        return (
            ((r & 4) << 6)
            | ((r & 2) << 6)
            | ((r >> 2) & 0x78)
            | ((r & 1) << 2)
            | ((r >> 3) & 3)
        )

    copies[3].wait()
    rows_ref[...] = permuted_rows(hop_ref[1], source)


def step_one(amplitudes, hop_blocks, coupling_seed):
    place = lax.axis_index(AXES).astype(jnp.int32).reshape(1)
    (coupling_seed,) = in_hbm(coupling_seed)
    smem = pl.BlockSpec(memory_space=pltpu.SMEM)
    vmem = pl.BlockSpec(memory_space=pltpu.VMEM)
    hbm = pl.BlockSpec(memory_space=pltpu.HBM)
    out, rows, base, side = pl.pallas_call(
        first_kernel,
        in_specs=[smem, smem, hbm, hbm],
        out_specs=[vmem, vmem, vmem, vmem],
        out_shape=[
            jax.ShapeDtypeStruct((4, 32, 32, 128), jnp.bfloat16),
            jax.ShapeDtypeStruct((512, 512), jnp.bfloat16),
            jax.ShapeDtypeStruct((512, 128), jnp.float32),
            jax.ShapeDtypeStruct((8, 4, 8, 128), jnp.float32),
        ],
        scratch_shapes=[
            pltpu.VMEM((2, 512, 512), jnp.bfloat16),
            pltpu.VMEM((2, 512, 512), jnp.bfloat16),
            pltpu.SemaphoreType.DMA((4,)),
        ],
        cost_estimate=pl.CostEstimate(
            flops=2 * 512 * 512 * 2048, bytes_accessed=5 << 19, transcendentals=1 << 17
        ),
        name="first",
        compiler_params=pltpu.CompilerParams(vmem_limit_bytes=16 << 20),
    )(coupling_seed, place, *in_hbm(amplitudes, hop_blocks))
    return out.reshape(128, 32, 128), rows, base, side


def gathered(moved_ref, g):
    z1, yh = g >> 2, g & 3
    return jnp.concatenate(
        [moved_ref[x, yh, zh, z1, core] for zh in range(2) for core in range(2) for x in range(4)],
        axis=0,
    )


def second_kernel(moved_ref, rows_ref, base_ref, side_ref, out_ref):
    base = base_ref[...].reshape(4, 16, 8, 128)
    for half in range(4):
        data = jnp.concatenate(
            [gathered(moved_ref, half * 2 + g) for g in range(2)], axis=1
        )
        second = product(rows_ref[...], data, NN)
        for b in range(2):
            g = half * 2 + b
            part = second[:, b * 128 : (b + 1) * 128].reshape(4, 16, 8, 128)
            mixed = part * (base * side_ref[g][:, None])
            out_ref[:, g] = mixed.reshape(16, 32, 128).astype(jnp.bfloat16)


def step_two(moved, rows, base, side):
    out = pl.pallas_call(
        second_kernel,
        grid=(1,),
        in_specs=[
            pl.BlockSpec((4, 4, 2, 2, 2, 32, 128), lambda i: (0, 0, 0, 0, 0, 0, 0)),
            pl.BlockSpec((512, 512), lambda i: (0, 0)),
            pl.BlockSpec((512, 128), lambda i: (0, 0)),
            pl.BlockSpec((8, 4, 8, 128), lambda i: (i, 0, 0, 0)),
        ],
        out_specs=pl.BlockSpec((16, 8, 32, 128), lambda i: (0, i, 0, 0)),
        out_shape=jax.ShapeDtypeStruct((16, 8, 32, 128), jnp.bfloat16),
        cost_estimate=pl.CostEstimate(
            flops=2 * 512 * 512 * 1024, bytes_accessed=3 << 20, transcendentals=0
        ),
        name="second",
        compiler_params=pltpu.CompilerParams(vmem_limit_bytes=16 << 20),
    )(moved.reshape(4, 4, 2, 2, 2, 32, 128), rows, base, side)
    return out.reshape(16, 256, 128)


def third_kernel(moved_ref, low_ref, high_ref, out_ref, held_ref):
    for step in range(4):
        data = jnp.concatenate([moved_ref[x, step] for x in range(4)], axis=1)
        third = product(data, low_ref[0], NT)
        at = (step >> 1) * 128 + (step & 1) * 16
        for top in range(4):
            lanes = slice(top * 128, (top + 1) * 128)
            parts = [
                jnp.concatenate(
                    [third[(g * 4 + j) * 8 : (g * 4 + j) * 8 + 8, lanes] for g in range(8)], axis=0
                )
                for j in range(4)
            ]
            swapped = swap_groups(parts)
            for j in range(4):
                for g in range(8):
                    where = (at + (g >> 2) * 256 + (g & 3) * 32 + top * 4 + j) * 8
                    held_ref[where : where + 8, :] = swapped[j][g * 8 : g * 8 + 8]
    for step in range(4):
        data = jnp.concatenate(
            [
                held_ref[pl.ds(step * 2 + b, 512, stride=8), :].astype(jnp.bfloat16)
                for b in range(2)
            ],
            axis=1,
        )
        fourth = product(high_ref[0], data, NN).astype(jnp.bfloat16)
        for b in range(2):
            for r in range(32):
                d13, d12, mid, d9 = r >> 4, (r >> 3) & 1, (r >> 1) & 3, r & 1
                out_ref[mid, d9, step >> 1, d13, d12, step & 1, b] = fourth[
                    r * 16 : r * 16 + 16, b * 128 : (b + 1) * 128
                ]


def step_three_four(moved, hop_blocks):
    out = pl.pallas_call(
        third_kernel,
        grid=(1,),
        in_specs=[
            pl.BlockSpec((4, 4, 256, 128), lambda i: (0, 0, 0, 0)),
            pl.BlockSpec((1, 512, 512), lambda i: (2, 0, 0)),
            pl.BlockSpec((1, 512, 512), lambda i: (3, 0, 0)),
        ],
        out_specs=pl.BlockSpec(
            (4, 2, 2, 2, 2, 2, 2, 16, 128), lambda i: (0, 0, 0, 0, 0, 0, 0, 0, 0)
        ),
        out_shape=jax.ShapeDtypeStruct((4, 2, 2, 2, 2, 2, 2, 16, 128), jnp.bfloat16),
        scratch_shapes=[pltpu.VMEM((4096, 128), jnp.float32)],
        cost_estimate=pl.CostEstimate(
            flops=4 * 512 * 512 * 1024, bytes_accessed=3 << 20, transcendentals=0
        ),
        name="third",
        compiler_params=pltpu.CompilerParams(vmem_limit_bytes=16 << 20),
    )(moved.reshape(4, 4, 256, 128), hop_blocks, hop_blocks)
    return out.reshape(128, 32, 128)


def last_kernel(moved_ref, out_hbm, held_ref, out_ref, sems):
    row = lax.broadcasted_iota(jnp.int32, (128, 128), 0)
    col = lax.broadcasted_iota(jnp.int32, (128, 128), 1)
    eye = jnp.where(row == col, 1.0, 0.0).astype(jnp.bfloat16)
    copies = []
    for pair in range(4):
        u9, u8 = pair >> 1, pair & 1
        for low in range(32):
            block = moved_ref[low >> 3, u8, (low >> 2) & 1, (low >> 1) & 1, u9, low & 1]
            for u7 in range(2):
                at = ((pair * 2 + u7) * 32 + low) * 16
                held_ref[at : at + 16, :] = block[u7 * 16 : u7 * 16 + 16].astype(jnp.float32)
        for u7 in range(2):
            for top in range(4):
                parts = [
                    held_ref[pl.ds((pair * 2 + u7) * 512 + top * 4 + j, 32, stride=16), :]
                    for j in range(4)
                ]
                tile = jnp.concatenate(swap_groups(parts), axis=0).astype(jnp.bfloat16)
                out_ref[pair, top * 128 : (top + 1) * 128, u7 * 128 : (u7 + 1) * 128] = product(
                    eye, tile, NT
                ).astype(jnp.bfloat16)
        copy = pltpu.make_async_copy(
            out_ref.at[pair], out_hbm.at[:, pair * 256 : (pair + 1) * 256], sems.at[pair]
        )
        copy.start()
        copies.append(copy)
    for copy in copies:
        copy.wait()


def finish(moved):
    return pl.pallas_call(
        last_kernel,
        in_specs=[pl.BlockSpec(memory_space=pltpu.VMEM)],
        out_specs=pl.BlockSpec(memory_space=pltpu.HBM),
        out_shape=jax.ShapeDtypeStruct((512, 1024), jnp.bfloat16),
        scratch_shapes=[
            pltpu.VMEM((4096, 128), jnp.float32),
            pltpu.VMEM((4, 512, 256), jnp.bfloat16),
            pltpu.SemaphoreType.DMA((4,)),
        ],
        name="last",
        compiler_params=pltpu.CompilerParams(vmem_limit_bytes=16 << 20),
    )(moved.reshape(4, 2, 2, 2, 2, 2, 32, 128))


def on_device(amplitudes, hop_blocks, coupling_seed):
    sent, rows, base, side = step_one(amplitudes, hop_blocks, coupling_seed)
    sent = exchange(sent, EX1)
    sent = exchange(step_two(sent, rows, base, side), EX2)
    sent = exchange(step_three_four(sent, hop_blocks), EX3)
    return finish(sent)


def solution(mesh):
    fine = Mesh(mesh.devices.reshape(SIZES), AXES)
    spec = P(("z1", "z0", "yh", "y0"), ("zh", "core", "x"))
    return jax.shard_map(
        on_device, mesh=fine, in_specs=(spec, P(), P()), out_specs=spec, check_vma=False
    )
```

```python
import jax
import jax.numpy as jnp
from jax import lax
from jax.experimental import pallas as pl
from jax.experimental.pallas import tpu as pltpu
from jax.sharding import Mesh, PartitionSpec as P

BLOCK = 512
SITES = 14
COUPLING = 0.06

AXES = ("zh", "core", "x", "z1", "z0", "yh", "y0")
SIZES = (2, 2, 4, 2, 2, 4, 2)
EX1 = ("x", "yh", "zh", "z1", "core")
EX2 = ("x", "z0", "y0")
EX3 = ("yh", "y0", "zh", "z1", "z0", "core")

NT = (((1,), (1,)), ((), ()))
NN = (((1,), (0,)), ((), ()))


def order_one():
    members = []
    for r in range(128):
        a, b, c, core = (r >> 1) & 3, (r >> 3) & 3, r >> 5, r & 1
        x, y, z = a, (b - a) & 3, (c + a) & 3
        members.append((((x * 4 + y) * 4 + z) << 1) | core)
    return members


def order_three():
    members = []
    for r in range(128):
        a, b, core = (r >> 1) & 7, r >> 4, r & 1
        y, z = (b + 3 * a) & 7, (3 * a) & 7
        members.append(((y * 8 + z) << 1) | core)
    return members


MEMBERS1, MEMBERS3 = order_one(), order_three()
SLOT1 = [MEMBERS1.index(m) for m in range(128)]
SLOT3 = [MEMBERS3.index(m) for m in range(128)]


def exchange(value, axes, members=None):
    groups = None if members is None else [members]
    return lax.all_to_all(
        value, axes, split_axis=0, concat_axis=0, tiled=True, axis_index_groups=groups
    )


def product(left, right, dims):
    return lax.dot_general(left, right, dims, preferred_element_type=jnp.float32)


def swap_groups(parts):
    group = lax.broadcasted_iota(jnp.int32, parts[0].shape, 1) >> 5
    is_group = [group == q for q in range(3)]

    def choose(values):
        out = values[3]
        for q in range(3):
            out = jnp.where(is_group[q], values[q], out)
        return out

    turned = []
    for m in range(4):
        held = choose([parts[(q + m) & 3] for q in range(4)])
        turned.append(held if m == 0 else pltpu.roll(held, 32 * m, 1))
    return [choose([turned[(q - a) & 3] for q in range(4)]) for a in range(4)]


def in_hbm(*arrays):
    return [pltpu.with_memory_space_constraint(a, pltpu.HBM) for a in arrays]


def permuted_rows(matrix, source):
    row = lax.broadcasted_iota(jnp.int32, (BLOCK, BLOCK), 0)
    col = lax.broadcasted_iota(jnp.int32, (BLOCK, BLOCK), 1)
    pick = jnp.where(col == source(row), 1.0, 0.0).astype(jnp.bfloat16)
    return product(pick, matrix, NN).astype(jnp.bfloat16)


def first_kernel(
    seed_ref, dev_ref, x_hbm, hop_hbm, out_ref, rows_ref, base_ref, side_ref, x_ref, hop_ref, sems
):
    copies = [
        pltpu.make_async_copy(hop_hbm.at[0], hop_ref.at[0], sems.at[0]),
        pltpu.make_async_copy(x_hbm.at[:, 0:512], x_ref.at[0], sems.at[1]),
        pltpu.make_async_copy(x_hbm.at[:, 512:1024], x_ref.at[1], sems.at[2]),
        pltpu.make_async_copy(hop_hbm.at[1], hop_ref.at[1], sems.at[3]),
    ]
    for copy in copies:
        copy.start()

    cost = [COUPLING * seed_ref[i].astype(jnp.float32) for i in range(SITES)]
    place = dev_ref[0]

    def at(shift):
        return ((place >> shift) & 1).astype(jnp.float32)

    zh, core, x1, x0, z1, z0, y2, y1, y0 = [at(8 - b) for b in range(9)]
    row = lax.broadcasted_iota(jnp.int32, (BLOCK, 128), 0)
    lane = lax.broadcasted_iota(jnp.int32, (BLOCK, 128), 1)

    def bit(index, shift):
        return ((index >> shift) & 1).astype(jnp.float32)

    energy = (cost[12] * z0) * bit(row, 1) + (cost[9] * y0) * bit(row, 6)
    energy += (cost[8] * x1) * bit(row, 5) + (cost[7] * x0) * bit(row, 0)
    energy += cost[6] * (bit(row, 4) * bit(lane, 6)) + cost[5] * (bit(row, 3) * bit(lane, 5))
    for site, held in enumerate((core, z1, zh, y1, y2)):
        energy += (cost[site] * held) * bit(lane, site)
    base_ref[...] = jnp.exp(-energy)
    small = lax.broadcasted_iota(jnp.int32, (8, 128), 0)
    for g in range(8):
        for top in range(4):
            extra = bit(small, 2) * (cost[13] * float(g >> 2))
            extra += cost[11] * float(((g >> 1) & 1) * (top >> 1))
            extra += cost[10] * float((g & 1) * (top & 1))
            side_ref[g, top] = jnp.exp(-extra)

    copies[0].wait()
    rows = permuted_rows(hop_ref[0], lambda r: ((r & 15) << 5) | (r >> 4))
    for u9 in range(2):
        copies[1 + u9].wait()
        first = product(rows, x_ref[u9], NT).astype(jnp.bfloat16)
        for x in range(4):
            for low in range(32):
                out_ref[SLOT1[x * 32 + low], u9 * 16 : (u9 + 1) * 16] = first[
                    low * 16 : low * 16 + 16, x * 128 : (x + 1) * 128
                ]

    def source(r):
        return (
            ((r & 4) << 6)
            | ((r & 2) << 6)
            | ((r >> 2) & 0x78)
            | ((r & 1) << 2)
            | ((r >> 3) & 3)
        )

    copies[3].wait()
    rows_ref[...] = permuted_rows(hop_ref[1], source)


def step_one(amplitudes, hop_blocks, coupling_seed):
    place = lax.axis_index(AXES).astype(jnp.int32).reshape(1)
    (coupling_seed,) = in_hbm(coupling_seed)
    smem = pl.BlockSpec(memory_space=pltpu.SMEM)
    vmem = pl.BlockSpec(memory_space=pltpu.VMEM)
    hbm = pl.BlockSpec(memory_space=pltpu.HBM)
    out, rows, base, side = pl.pallas_call(
        first_kernel,
        in_specs=[smem, smem, hbm, hbm],
        out_specs=[vmem, vmem, vmem, vmem],
        out_shape=[
            jax.ShapeDtypeStruct((128, 32, 128), jnp.bfloat16),
            jax.ShapeDtypeStruct((512, 512), jnp.bfloat16),
            jax.ShapeDtypeStruct((512, 128), jnp.float32),
            jax.ShapeDtypeStruct((8, 4, 8, 128), jnp.float32),
        ],
        scratch_shapes=[
            pltpu.VMEM((2, 512, 512), jnp.bfloat16),
            pltpu.VMEM((2, 512, 512), jnp.bfloat16),
            pltpu.SemaphoreType.DMA((4,)),
        ],
        cost_estimate=pl.CostEstimate(
            flops=2 * 512 * 512 * 2048, bytes_accessed=5 << 19, transcendentals=1 << 17
        ),
        name="first",
        compiler_params=pltpu.CompilerParams(vmem_limit_bytes=16 << 20),
    )(coupling_seed, place, *in_hbm(amplitudes, hop_blocks))
    return out, rows, base, side


def gathered(moved_ref, g):
    z1, yh = g >> 2, g & 3
    return jnp.concatenate(
        [
            moved_ref[SLOT1[x * 32 + yh * 8 + zh * 4 + z1 * 2 + core]]
            for zh in range(2)
            for core in range(2)
            for x in range(4)
        ],
        axis=0,
    )


def second_kernel(moved_ref, rows_ref, base_ref, side_ref, out_ref):
    base = base_ref[...].reshape(4, 16, 8, 128)
    for half in range(4):
        data = jnp.concatenate(
            [gathered(moved_ref, half * 2 + g) for g in range(2)], axis=1
        )
        second = product(rows_ref[...], data, NN)
        for b in range(2):
            g = half * 2 + b
            part = second[:, b * 128 : (b + 1) * 128].reshape(4, 16, 8, 128)
            mixed = part * (base * side_ref[g][:, None])
            out_ref[:, g] = mixed.reshape(16, 32, 128).astype(jnp.bfloat16)


def step_two(moved, rows, base, side):
    out = pl.pallas_call(
        second_kernel,
        grid=(1,),
        in_specs=[
            pl.BlockSpec((128, 32, 128), lambda i: (0, 0, 0)),
            pl.BlockSpec((512, 512), lambda i: (0, 0)),
            pl.BlockSpec((512, 128), lambda i: (0, 0)),
            pl.BlockSpec((8, 4, 8, 128), lambda i: (i, 0, 0, 0)),
        ],
        out_specs=pl.BlockSpec((16, 8, 32, 128), lambda i: (0, i, 0, 0)),
        out_shape=jax.ShapeDtypeStruct((16, 8, 32, 128), jnp.bfloat16),
        cost_estimate=pl.CostEstimate(
            flops=2 * 512 * 512 * 1024, bytes_accessed=3 << 20, transcendentals=0
        ),
        name="second",
        compiler_params=pltpu.CompilerParams(vmem_limit_bytes=16 << 20),
    )(moved, rows, base, side)
    return out.reshape(16, 256, 128)


def third_kernel(moved_ref, low_ref, high_ref, out_ref, held_ref):
    for step in range(4):
        data = jnp.concatenate([moved_ref[x, step] for x in range(4)], axis=1)
        third = product(data, low_ref[0], NT)
        at = (step >> 1) * 128 + (step & 1) * 16
        for top in range(4):
            lanes = slice(top * 128, (top + 1) * 128)
            parts = [
                jnp.concatenate(
                    [third[(g * 4 + j) * 8 : (g * 4 + j) * 8 + 8, lanes] for g in range(8)], axis=0
                )
                for j in range(4)
            ]
            swapped = swap_groups(parts)
            for j in range(4):
                for g in range(8):
                    where = (at + (g >> 2) * 256 + (g & 3) * 32 + top * 4 + j) * 8
                    held_ref[where : where + 8, :] = swapped[j][g * 8 : g * 8 + 8]
    for step in range(4):
        data = jnp.concatenate(
            [
                held_ref[pl.ds(step * 2 + b, 512, stride=8), :].astype(jnp.bfloat16)
                for b in range(2)
            ],
            axis=1,
        )
        fourth = product(high_ref[0], data, NN).astype(jnp.bfloat16)
        for b in range(2):
            for r in range(32):
                d13, d12, mid, d9 = r >> 4, (r >> 3) & 1, (r >> 1) & 3, r & 1
                member = mid * 32 + d9 * 16 + (step >> 1) * 8 + d13 * 4 + d12 * 2 + (step & 1)
                out_ref[SLOT3[member], b * 16 : b * 16 + 16] = fourth[
                    r * 16 : r * 16 + 16, b * 128 : (b + 1) * 128
                ]


def step_three_four(moved, hop_blocks):
    out = pl.pallas_call(
        third_kernel,
        grid=(1,),
        in_specs=[
            pl.BlockSpec((4, 4, 256, 128), lambda i: (0, 0, 0, 0)),
            pl.BlockSpec((1, 512, 512), lambda i: (2, 0, 0)),
            pl.BlockSpec((1, 512, 512), lambda i: (3, 0, 0)),
        ],
        out_specs=pl.BlockSpec((128, 32, 128), lambda i: (0, 0, 0)),
        out_shape=jax.ShapeDtypeStruct((128, 32, 128), jnp.bfloat16),
        scratch_shapes=[pltpu.VMEM((4096, 128), jnp.float32)],
        cost_estimate=pl.CostEstimate(
            flops=4 * 512 * 512 * 1024, bytes_accessed=3 << 20, transcendentals=0
        ),
        name="third",
        compiler_params=pltpu.CompilerParams(vmem_limit_bytes=16 << 20),
    )(moved.reshape(4, 4, 256, 128), hop_blocks, hop_blocks)
    return out


def last_kernel(moved_ref, out_hbm, held_ref, out_ref, sems):
    row = lax.broadcasted_iota(jnp.int32, (128, 128), 0)
    col = lax.broadcasted_iota(jnp.int32, (128, 128), 1)
    eye = jnp.where(row == col, 1.0, 0.0).astype(jnp.bfloat16)
    copies = []
    for pair in range(4):
        u9, u8 = pair >> 1, pair & 1
        for low in range(32):
            member = (low >> 3) * 32 + u8 * 16 + ((low >> 1) & 3) * 4 + u9 * 2 + (low & 1)
            block = moved_ref[SLOT3[member]]
            for u7 in range(2):
                at = ((pair * 2 + u7) * 32 + low) * 16
                held_ref[at : at + 16, :] = block[u7 * 16 : u7 * 16 + 16].astype(jnp.float32)
        for u7 in range(2):
            for top in range(4):
                parts = [
                    held_ref[pl.ds((pair * 2 + u7) * 512 + top * 4 + j, 32, stride=16), :]
                    for j in range(4)
                ]
                tile = jnp.concatenate(swap_groups(parts), axis=0).astype(jnp.bfloat16)
                out_ref[pair, top * 128 : (top + 1) * 128, u7 * 128 : (u7 + 1) * 128] = product(
                    eye, tile, NT
                ).astype(jnp.bfloat16)
        copy = pltpu.make_async_copy(
            out_ref.at[pair], out_hbm.at[:, pair * 256 : (pair + 1) * 256], sems.at[pair]
        )
        copy.start()
        copies.append(copy)
    for copy in copies:
        copy.wait()


def finish(moved):
    return pl.pallas_call(
        last_kernel,
        in_specs=[pl.BlockSpec(memory_space=pltpu.VMEM)],
        out_specs=pl.BlockSpec(memory_space=pltpu.HBM),
        out_shape=jax.ShapeDtypeStruct((512, 1024), jnp.bfloat16),
        scratch_shapes=[
            pltpu.VMEM((4096, 128), jnp.float32),
            pltpu.VMEM((4, 512, 256), jnp.bfloat16),
            pltpu.SemaphoreType.DMA((4,)),
        ],
        name="last",
        compiler_params=pltpu.CompilerParams(vmem_limit_bytes=16 << 20),
    )(moved)


def on_device(amplitudes, hop_blocks, coupling_seed):
    sent, rows, base, side = step_one(amplitudes, hop_blocks, coupling_seed)
    sent = exchange(sent, EX1, MEMBERS1)
    sent = exchange(step_two(sent, rows, base, side), EX2)
    sent = exchange(step_three_four(sent, hop_blocks), EX3, MEMBERS3)
    return finish(sent)


def solution(mesh):
    fine = Mesh(mesh.devices.reshape(SIZES), AXES)
    spec = P(("z1", "z0", "yh", "y0"), ("zh", "core", "x"))
    return jax.shard_map(
        on_device, mesh=fine, in_specs=(spec, P(), P()), out_specs=spec, check_vma=False
    )
```

```python
import jax
import jax.numpy as jnp
from jax import lax
from jax.experimental import pallas as pl
from jax.experimental.pallas import tpu as pltpu
from jax.sharding import Mesh, PartitionSpec as P

BLOCK = 512
SITES = 14
COUPLING = 0.06

AXES = ("zh", "core", "x", "z1", "z0", "yh", "y0")
SIZES = (2, 2, 4, 2, 2, 4, 2)
EX1 = ("x", "yh", "zh", "z1", "core")
EX2 = ("x", "z0", "y0")
EX3 = ("core", "yh", "y0", "zh", "z1", "z0")

NT = (((1,), (1,)), ((), ()))
NN = (((1,), (0,)), ((), ()))


SLOT3 = [(m & 1) * 64 + (m >> 1) for m in range(128)]


def exchange(value, axes):
    return lax.all_to_all(value, axes, split_axis=0, concat_axis=0, tiled=True)


def product(left, right, dims):
    return lax.dot_general(left, right, dims, preferred_element_type=jnp.float32)


def swap_groups(parts):
    group = lax.broadcasted_iota(jnp.int32, parts[0].shape, 1) >> 5
    is_group = [group == q for q in range(3)]

    def choose(values):
        out = values[3]
        for q in range(3):
            out = jnp.where(is_group[q], values[q], out)
        return out

    turned = []
    for m in range(4):
        held = choose([parts[(q + m) & 3] for q in range(4)])
        turned.append(held if m == 0 else pltpu.roll(held, 32 * m, 1))
    return [choose([turned[(q - a) & 3] for q in range(4)]) for a in range(4)]


def in_hbm(*arrays):
    return [pltpu.with_memory_space_constraint(a, pltpu.HBM) for a in arrays]


def permuted_rows(matrix, inner, outer):
    row = lax.broadcasted_iota(jnp.int32, (16, BLOCK), 0)
    col = lax.broadcasted_iota(jnp.int32, (16, BLOCK), 1)
    apart = col - inner(row)
    pick = jnp.concatenate(
        [jnp.where(apart == outer(t), 1.0, 0.0).astype(jnp.bfloat16) for t in range(32)], axis=0
    )
    return product(pick, matrix, NN).astype(jnp.bfloat16)


def first_kernel(
    seed_ref, dev_ref, x_hbm, hop_hbm, out_ref, rows_ref, base_ref, side_ref, x_ref, hop_ref, sems
):
    copies = [
        pltpu.make_async_copy(hop_hbm.at[0], hop_ref.at[0], sems.at[0]),
        pltpu.make_async_copy(x_hbm.at[:, 0:512], x_ref.at[0], sems.at[1]),
        pltpu.make_async_copy(x_hbm.at[:, 512:1024], x_ref.at[1], sems.at[2]),
        pltpu.make_async_copy(hop_hbm.at[1], hop_ref.at[1], sems.at[3]),
    ]
    for copy in copies:
        copy.start()

    cost = [COUPLING * seed_ref[i].astype(jnp.float32) for i in range(SITES)]
    place = dev_ref[0]

    def at(shift):
        return ((place >> shift) & 1).astype(jnp.float32)

    zh, core, x1, x0, z1, z0, y2, y1, y0 = [at(8 - b) for b in range(9)]
    row = lax.broadcasted_iota(jnp.int32, (128, 128), 0)
    lane = lax.broadcasted_iota(jnp.int32, (128, 128), 1)

    def bit(index, shift):
        return ((index >> shift) & 1).astype(jnp.float32)

    energy = (cost[12] * z0) * bit(row, 1) + (cost[9] * y0) * bit(row, 6)
    energy += (cost[8] * x1) * bit(row, 5) + (cost[7] * x0) * bit(row, 0)
    energy += cost[6] * (bit(row, 4) * bit(lane, 6)) + cost[5] * (bit(row, 3) * bit(lane, 5))
    for site, held in enumerate((core, z1, zh, y1, y2)):
        energy += (cost[site] * held) * bit(lane, site)
    base_ref[...] = jnp.exp(-energy)
    small = lax.broadcasted_iota(jnp.int32, (8, 128), 0)
    for g in range(8):
        for top in range(4):
            extra = bit(small, 2) * (cost[13] * float(g >> 2))
            extra += cost[11] * float(((g >> 1) & 1) * (top >> 1))
            extra += cost[10] * float((g & 1) * (top & 1))
            side_ref[g, top] = jnp.exp(-extra)

    copies[0].wait()
    rows = permuted_rows(hop_ref[0], lambda s: s << 5, lambda t: t)
    for u9 in range(2):
        copies[1 + u9].wait()
        first = product(rows, x_ref[u9], NT).astype(jnp.bfloat16)
        for x in range(4):
            for low in range(32):
                out_ref[x * 32 + low, u9 * 16 : (u9 + 1) * 16] = first[
                    low * 16 : low * 16 + 16, x * 128 : (x + 1) * 128
                ]

    copies[3].wait()
    rows_ref[...] = permuted_rows(
        hop_ref[1],
        lambda s: ((s & 6) << 6) + ((s & 1) << 2) + (s >> 3),
        lambda t: ((t >> 1) << 3) + ((t & 1) << 1),
    )


def step_one(amplitudes, hop_blocks, coupling_seed):
    place = lax.axis_index(AXES).astype(jnp.int32).reshape(1)
    (coupling_seed,) = in_hbm(coupling_seed)
    smem = pl.BlockSpec(memory_space=pltpu.SMEM)
    vmem = pl.BlockSpec(memory_space=pltpu.VMEM)
    hbm = pl.BlockSpec(memory_space=pltpu.HBM)
    out, rows, base, side = pl.pallas_call(
        first_kernel,
        in_specs=[smem, smem, hbm, hbm],
        out_specs=[vmem, vmem, vmem, vmem],
        out_shape=[
            jax.ShapeDtypeStruct((128, 32, 128), jnp.bfloat16),
            jax.ShapeDtypeStruct((512, 512), jnp.bfloat16),
            jax.ShapeDtypeStruct((128, 128), jnp.float32),
            jax.ShapeDtypeStruct((8, 4, 8, 128), jnp.float32),
        ],
        scratch_shapes=[
            pltpu.VMEM((2, 512, 512), jnp.bfloat16),
            pltpu.VMEM((2, 512, 512), jnp.bfloat16),
            pltpu.SemaphoreType.DMA((4,)),
        ],
        cost_estimate=pl.CostEstimate(
            flops=2 * 512 * 512 * 2048, bytes_accessed=5 << 19, transcendentals=1 << 17
        ),
        name="first",
        compiler_params=pltpu.CompilerParams(vmem_limit_bytes=16 << 20),
    )(coupling_seed, place, *in_hbm(amplitudes, hop_blocks))
    return out, rows, base, side


def gathered(moved_ref, g):
    z1, yh = g >> 2, g & 3
    return jnp.concatenate(
        [
            moved_ref[x * 32 + yh * 8 + zh * 4 + z1 * 2 + core]
            for zh in range(2)
            for core in range(2)
            for x in range(4)
        ],
        axis=0,
    )


def second_kernel(moved_ref, rows_ref, base_ref, side_ref, out_ref):
    base = base_ref[...].reshape(1, 16, 8, 128)
    for half in range(4):
        data = jnp.concatenate(
            [gathered(moved_ref, half * 2 + g) for g in range(2)], axis=1
        )
        second = product(rows_ref[...], data, NN)
        for b in range(2):
            g = half * 2 + b
            part = second[:, b * 128 : (b + 1) * 128].reshape(4, 16, 8, 128)
            mixed = part * (base * side_ref[g][:, None])
            out_ref[:, g] = mixed.reshape(16, 32, 128).astype(jnp.bfloat16)


def step_two(moved, rows, base, side):
    out = pl.pallas_call(
        second_kernel,
        grid=(1,),
        in_specs=[
            pl.BlockSpec((128, 32, 128), lambda i: (0, 0, 0)),
            pl.BlockSpec((512, 512), lambda i: (0, 0)),
            pl.BlockSpec((128, 128), lambda i: (0, 0)),
            pl.BlockSpec((8, 4, 8, 128), lambda i: (i, 0, 0, 0)),
        ],
        out_specs=pl.BlockSpec((16, 8, 32, 128), lambda i: (0, i, 0, 0)),
        out_shape=jax.ShapeDtypeStruct((16, 8, 32, 128), jnp.bfloat16),
        cost_estimate=pl.CostEstimate(
            flops=2 * 512 * 512 * 1024, bytes_accessed=3 << 20, transcendentals=0
        ),
        name="second",
        compiler_params=pltpu.CompilerParams(vmem_limit_bytes=16 << 20),
    )(moved, rows, base, side)
    return out.reshape(16, 256, 128)


def third_kernel(moved_ref, low_ref, high_ref, out_ref, held_ref):
    for step in range(4):
        data = jnp.concatenate([moved_ref[x, step] for x in range(4)], axis=1)
        third = product(data, low_ref[0], NT)
        at = (step >> 1) * 128 + (step & 1) * 16
        for top in range(4):
            lanes = slice(top * 128, (top + 1) * 128)
            parts = [
                jnp.concatenate(
                    [third[(g * 4 + j) * 8 : (g * 4 + j) * 8 + 8, lanes] for g in range(8)], axis=0
                )
                for j in range(4)
            ]
            swapped = swap_groups(parts)
            for j in range(4):
                for g in range(8):
                    where = (at + (g >> 2) * 256 + (g & 3) * 32 + top * 4 + j) * 8
                    held_ref[where : where + 8, :] = swapped[j][g * 8 : g * 8 + 8]
    for step in range(4):
        data = jnp.concatenate(
            [
                held_ref[pl.ds(step * 2 + b, 512, stride=8), :].astype(jnp.bfloat16)
                for b in range(2)
            ],
            axis=1,
        )
        fourth = product(high_ref[0], data, NN).astype(jnp.bfloat16)
        for b in range(2):
            for r in range(32):
                d13, d12, mid, d9 = r >> 4, (r >> 3) & 1, (r >> 1) & 3, r & 1
                member = mid * 32 + d9 * 16 + (step >> 1) * 8 + d13 * 4 + d12 * 2 + (step & 1)
                out_ref[SLOT3[member], b * 16 : b * 16 + 16] = fourth[
                    r * 16 : r * 16 + 16, b * 128 : (b + 1) * 128
                ]


def step_three_four(moved, hop_blocks):
    out = pl.pallas_call(
        third_kernel,
        grid=(1,),
        in_specs=[
            pl.BlockSpec((4, 4, 256, 128), lambda i: (0, 0, 0, 0)),
            pl.BlockSpec((1, 512, 512), lambda i: (2, 0, 0)),
            pl.BlockSpec((1, 512, 512), lambda i: (3, 0, 0)),
        ],
        out_specs=pl.BlockSpec((128, 32, 128), lambda i: (0, 0, 0)),
        out_shape=jax.ShapeDtypeStruct((128, 32, 128), jnp.bfloat16),
        scratch_shapes=[pltpu.VMEM((4096, 128), jnp.float32)],
        cost_estimate=pl.CostEstimate(
            flops=4 * 512 * 512 * 1024, bytes_accessed=3 << 20, transcendentals=0
        ),
        name="third",
        compiler_params=pltpu.CompilerParams(vmem_limit_bytes=16 << 20),
    )(moved.reshape(4, 4, 256, 128), hop_blocks, hop_blocks)
    return out


def last_kernel(moved_ref, out_hbm, held_ref, out_ref, sems):
    row = lax.broadcasted_iota(jnp.int32, (128, 128), 0)
    col = lax.broadcasted_iota(jnp.int32, (128, 128), 1)
    eye = jnp.where(row == col, 1.0, 0.0).astype(jnp.bfloat16)
    copies = []
    for pair in range(4):
        u9, u8 = pair >> 1, pair & 1
        for low in range(32):
            member = (low >> 3) * 32 + u8 * 16 + ((low >> 1) & 3) * 4 + u9 * 2 + (low & 1)
            block = moved_ref[SLOT3[member]]
            for u7 in range(2):
                at = ((pair * 2 + u7) * 32 + low) * 16
                held_ref[at : at + 16, :] = block[u7 * 16 : u7 * 16 + 16].astype(jnp.float32)
        for u7 in range(2):
            for top in range(4):
                parts = [
                    held_ref[pl.ds((pair * 2 + u7) * 512 + top * 4 + j, 32, stride=16), :]
                    for j in range(4)
                ]
                tile = jnp.concatenate(swap_groups(parts), axis=0).astype(jnp.bfloat16)
                out_ref[pair, top * 128 : (top + 1) * 128, u7 * 128 : (u7 + 1) * 128] = product(
                    eye, tile, NT
                ).astype(jnp.bfloat16)
        copy = pltpu.make_async_copy(
            out_ref.at[pair], out_hbm.at[:, pair * 256 : (pair + 1) * 256], sems.at[pair]
        )
        copy.start()
        copies.append(copy)
    for copy in copies:
        copy.wait()


def finish(moved):
    return pl.pallas_call(
        last_kernel,
        in_specs=[pl.BlockSpec(memory_space=pltpu.VMEM)],
        out_specs=pl.BlockSpec(memory_space=pltpu.HBM),
        out_shape=jax.ShapeDtypeStruct((512, 1024), jnp.bfloat16),
        scratch_shapes=[
            pltpu.VMEM((4096, 128), jnp.float32),
            pltpu.VMEM((4, 512, 256), jnp.bfloat16),
            pltpu.SemaphoreType.DMA((4,)),
        ],
        name="last",
        compiler_params=pltpu.CompilerParams(vmem_limit_bytes=16 << 20),
    )(moved)


def on_device(amplitudes, hop_blocks, coupling_seed):
    sent, rows, base, side = step_one(amplitudes, hop_blocks, coupling_seed)
    sent = exchange(sent, EX1)
    sent = exchange(step_two(sent, rows, base, side), EX2)
    sent = exchange(step_three_four(sent, hop_blocks), EX3)
    return finish(sent)


def solution(mesh):
    fine = Mesh(mesh.devices.reshape(SIZES), AXES)
    spec = P(("z1", "z0", "yh", "y0"), ("zh", "core", "x"))
    return jax.shard_map(
        on_device, mesh=fine, in_specs=(spec, P(), P()), out_specs=spec, check_vma=False
    )
```

```python
import jax
import jax.numpy as jnp
from jax import lax
from jax.experimental import pallas as pl
from jax.experimental.pallas import tpu as pltpu
from jax.sharding import Mesh, PartitionSpec as P

BLOCK = 512
SITES = 14
COUPLING = 0.06

AXES = ("zh", "core", "x", "z1", "z0", "yh", "y0")
SIZES = (2, 2, 4, 2, 2, 4, 2)
EX1 = ("x", "yh", "zh", "z1", "core")
EX2 = ("x", "z0", "y0")
EX3 = ("yh", "y0", "zh", "z1", "z0", "core")

NT = (((1,), (1,)), ((), ()))
NN = (((1,), (0,)), ((), ()))


def exchange(value, axes):
    return lax.all_to_all(value, axes, split_axis=0, concat_axis=0, tiled=True)


def product(left, right, dims):
    return lax.dot_general(left, right, dims, preferred_element_type=jnp.float32)


def swap_groups(parts):
    group = lax.broadcasted_iota(jnp.int32, parts[0].shape, 1) >> 5
    is_group = [group == q for q in range(3)]

    def choose(values):
        out = values[3]
        for q in range(3):
            out = jnp.where(is_group[q], values[q], out)
        return out

    turned = []
    for m in range(4):
        held = choose([parts[(q + m) & 3] for q in range(4)])
        turned.append(held if m == 0 else pltpu.roll(held, 32 * m, 1))
    return [choose([turned[(q - a) & 3] for q in range(4)]) for a in range(4)]


def in_hbm(*arrays):
    return [pltpu.with_memory_space_constraint(a, pltpu.HBM) for a in arrays]


def permuted_rows(matrix, inner, outer):
    row = lax.broadcasted_iota(jnp.int32, (16, BLOCK), 0)
    col = lax.broadcasted_iota(jnp.int32, (16, BLOCK), 1)
    apart = col - inner(row)
    pick = jnp.concatenate(
        [jnp.where(apart == outer(t), 1.0, 0.0).astype(jnp.bfloat16) for t in range(32)], axis=0
    )
    return product(pick, matrix, NN).astype(jnp.bfloat16)


def first_kernel(
    seed_ref, dev_ref, x_hbm, hop_hbm, out_ref, rows_ref, base_ref, side_ref, x_ref, hop_ref, sems
):
    copies = [
        pltpu.make_async_copy(hop_hbm.at[0], hop_ref.at[0], sems.at[0]),
        pltpu.make_async_copy(x_hbm.at[:, 0:512], x_ref.at[0], sems.at[1]),
        pltpu.make_async_copy(x_hbm.at[:, 512:1024], x_ref.at[1], sems.at[2]),
        pltpu.make_async_copy(hop_hbm.at[1], hop_ref.at[1], sems.at[3]),
    ]
    for copy in copies:
        copy.start()

    cost = [COUPLING * seed_ref[i].astype(jnp.float32) for i in range(SITES)]
    place = dev_ref[0]

    def at(shift):
        return ((place >> shift) & 1).astype(jnp.float32)

    zh, core, x1, x0, z1, z0, y2, y1, y0 = [at(8 - b) for b in range(9)]
    row = lax.broadcasted_iota(jnp.int32, (128, 128), 0)
    lane = lax.broadcasted_iota(jnp.int32, (128, 128), 1)

    def bit(index, shift):
        return ((index >> shift) & 1).astype(jnp.float32)

    energy = (cost[12] * z0) * bit(row, 1) + (cost[9] * y0) * bit(row, 6)
    energy += (cost[8] * x1) * bit(row, 5) + (cost[7] * x0) * bit(row, 0)
    energy += cost[6] * (bit(row, 4) * bit(lane, 6)) + cost[5] * (bit(row, 3) * bit(lane, 5))
    for site, held in enumerate((core, z1, zh, y1, y2)):
        energy += (cost[site] * held) * bit(lane, site)
    base_ref[...] = jnp.exp(-energy)
    small = lax.broadcasted_iota(jnp.int32, (8, 128), 0)
    for g in range(8):
        for top in range(4):
            extra = bit(small, 2) * (cost[13] * float(g >> 2))
            extra += cost[11] * float(((g >> 1) & 1) * (top >> 1))
            extra += cost[10] * float((g & 1) * (top & 1))
            side_ref[g, top] = jnp.exp(-extra)

    copies[0].wait()
    rows = permuted_rows(hop_ref[0], lambda s: s << 5, lambda t: t)
    for u9 in range(2):
        copies[1 + u9].wait()
        first = product(rows, x_ref[u9], NT).astype(jnp.bfloat16)
        for x in range(4):
            for low in range(32):
                out_ref[x * 32 + low, u9 * 16 : (u9 + 1) * 16] = first[
                    low * 16 : low * 16 + 16, x * 128 : (x + 1) * 128
                ]

    copies[3].wait()
    rows_ref[...] = permuted_rows(
        hop_ref[1],
        lambda s: ((s & 6) << 6) + ((s & 1) << 2) + (s >> 3),
        lambda t: ((t >> 1) << 3) + ((t & 1) << 1),
    )


def step_one(amplitudes, hop_blocks, coupling_seed):
    place = lax.axis_index(AXES).astype(jnp.int32).reshape(1)
    (coupling_seed,) = in_hbm(coupling_seed)
    smem = pl.BlockSpec(memory_space=pltpu.SMEM)
    vmem = pl.BlockSpec(memory_space=pltpu.VMEM)
    hbm = pl.BlockSpec(memory_space=pltpu.HBM)
    out, rows, base, side = pl.pallas_call(
        first_kernel,
        in_specs=[smem, smem, hbm, hbm],
        out_specs=[vmem, vmem, vmem, vmem],
        out_shape=[
            jax.ShapeDtypeStruct((128, 32, 128), jnp.bfloat16),
            jax.ShapeDtypeStruct((512, 512), jnp.bfloat16),
            jax.ShapeDtypeStruct((128, 128), jnp.float32),
            jax.ShapeDtypeStruct((8, 4, 8, 128), jnp.float32),
        ],
        scratch_shapes=[
            pltpu.VMEM((2, 512, 512), jnp.bfloat16),
            pltpu.VMEM((2, 512, 512), jnp.bfloat16),
            pltpu.SemaphoreType.DMA((4,)),
        ],
        cost_estimate=pl.CostEstimate(
            flops=2 * 512 * 512 * 2048, bytes_accessed=5 << 19, transcendentals=1 << 17
        ),
        name="first",
        compiler_params=pltpu.CompilerParams(vmem_limit_bytes=16 << 20),
    )(coupling_seed, place, *in_hbm(amplitudes, hop_blocks))
    return out, rows, base, side


def gathered(moved_ref, g):
    z1, yh = g >> 2, g & 3
    return jnp.concatenate(
        [
            moved_ref[x * 32 + yh * 8 + zh * 4 + z1 * 2 + core]
            for zh in range(2)
            for core in range(2)
            for x in range(4)
        ],
        axis=0,
    )


def second_kernel(moved_ref, rows_ref, base_ref, side_ref, out_ref):
    base = base_ref[...].reshape(1, 16, 8, 128)
    for half in range(4):
        data = jnp.concatenate(
            [gathered(moved_ref, half * 2 + g) for g in range(2)], axis=1
        )
        second = product(rows_ref[...], data, NN)
        for b in range(2):
            g = half * 2 + b
            part = second[:, b * 128 : (b + 1) * 128].reshape(4, 16, 8, 128)
            mixed = part * (base * side_ref[g][:, None])
            out_ref[:, g] = mixed.reshape(16, 32, 128).astype(jnp.bfloat16)


def step_two(moved, rows, base, side):
    out = pl.pallas_call(
        second_kernel,
        grid=(1,),
        in_specs=[
            pl.BlockSpec((128, 32, 128), lambda i: (0, 0, 0)),
            pl.BlockSpec((512, 512), lambda i: (0, 0)),
            pl.BlockSpec((128, 128), lambda i: (0, 0)),
            pl.BlockSpec((8, 4, 8, 128), lambda i: (i, 0, 0, 0)),
        ],
        out_specs=pl.BlockSpec((16, 8, 32, 128), lambda i: (0, i, 0, 0)),
        out_shape=jax.ShapeDtypeStruct((16, 8, 32, 128), jnp.bfloat16),
        cost_estimate=pl.CostEstimate(
            flops=2 * 512 * 512 * 1024, bytes_accessed=3 << 20, transcendentals=0
        ),
        name="second",
        compiler_params=pltpu.CompilerParams(vmem_limit_bytes=16 << 20),
    )(moved, rows, base, side)
    return out.reshape(16, 256, 128)


def third_kernel(moved_ref, low_ref, high_ref, out_ref, held_ref):
    for step in range(4):
        data = jnp.concatenate([moved_ref[x, step] for x in range(4)], axis=1)
        third = product(data, low_ref[0], NT)
        at = (step >> 1) * 128 + (step & 1) * 16
        for top in range(4):
            lanes = slice(top * 128, (top + 1) * 128)
            parts = [
                jnp.concatenate(
                    [third[(g * 4 + j) * 8 : (g * 4 + j) * 8 + 8, lanes] for g in range(8)], axis=0
                )
                for j in range(4)
            ]
            swapped = swap_groups(parts)
            for j in range(4):
                for g in range(8):
                    where = (at + (g >> 2) * 256 + (g & 3) * 32 + top * 4 + j) * 8
                    held_ref[where : where + 8, :] = swapped[j][g * 8 : g * 8 + 8]
    for step in range(4):
        data = jnp.concatenate(
            [
                held_ref[pl.ds(step * 2 + b, 512, stride=8), :].astype(jnp.bfloat16)
                for b in range(2)
            ],
            axis=1,
        )
        fourth = product(high_ref[0], data, NN).astype(jnp.bfloat16)
        for b in range(2):
            for r in range(32):
                d13, d12, mid, d9 = r >> 4, (r >> 3) & 1, (r >> 1) & 3, r & 1
                member = mid * 32 + d9 * 16 + (step >> 1) * 8 + d13 * 4 + d12 * 2 + (step & 1)
                out_ref[member, b * 16 : b * 16 + 16] = fourth[
                    r * 16 : r * 16 + 16, b * 128 : (b + 1) * 128
                ]


def step_three_four(moved, hop_blocks):
    out = pl.pallas_call(
        third_kernel,
        grid=(1,),
        in_specs=[
            pl.BlockSpec((4, 4, 256, 128), lambda i: (0, 0, 0, 0)),
            pl.BlockSpec((1, 512, 512), lambda i: (2, 0, 0)),
            pl.BlockSpec((1, 512, 512), lambda i: (3, 0, 0)),
        ],
        out_specs=pl.BlockSpec((128, 32, 128), lambda i: (0, 0, 0)),
        out_shape=jax.ShapeDtypeStruct((128, 32, 128), jnp.bfloat16),
        scratch_shapes=[pltpu.VMEM((4096, 128), jnp.float32)],
        cost_estimate=pl.CostEstimate(
            flops=4 * 512 * 512 * 1024, bytes_accessed=3 << 20, transcendentals=0
        ),
        name="third",
        compiler_params=pltpu.CompilerParams(vmem_limit_bytes=16 << 20),
    )(moved.reshape(4, 4, 256, 128), hop_blocks, hop_blocks)
    return out


def last_kernel(moved_ref, out_hbm, held_ref, out_ref, sems):
    row = lax.broadcasted_iota(jnp.int32, (128, 128), 0)
    col = lax.broadcasted_iota(jnp.int32, (128, 128), 1)
    eye = jnp.where(row == col, 1.0, 0.0).astype(jnp.bfloat16)
    copies = []
    for pair in range(4):
        u9, u8 = pair >> 1, pair & 1
        for low in range(32):
            member = (low >> 3) * 32 + u8 * 16 + ((low >> 1) & 3) * 4 + u9 * 2 + (low & 1)
            block = moved_ref[member]
            for u7 in range(2):
                at = ((pair * 2 + u7) * 32 + low) * 16
                held_ref[at : at + 16, :] = block[u7 * 16 : u7 * 16 + 16].astype(jnp.float32)
        for u7 in range(2):
            for top in range(4):
                parts = [
                    held_ref[pl.ds((pair * 2 + u7) * 512 + top * 4 + j, 32, stride=16), :].astype(jnp.bfloat16)
                    for j in range(4)
                ]
                tile = jnp.concatenate(swap_groups(parts), axis=0)
                out_ref[pair, top * 128 : (top + 1) * 128, u7 * 128 : (u7 + 1) * 128] = product(
                    eye, tile, NT
                ).astype(jnp.bfloat16)
        copy = pltpu.make_async_copy(
            out_ref.at[pair], out_hbm.at[:, pair * 256 : (pair + 1) * 256], sems.at[pair]
        )
        copy.start()
        copies.append(copy)
    for copy in copies:
        copy.wait()


def finish(moved):
    return pl.pallas_call(
        last_kernel,
        in_specs=[pl.BlockSpec(memory_space=pltpu.VMEM)],
        out_specs=pl.BlockSpec(memory_space=pltpu.HBM),
        out_shape=jax.ShapeDtypeStruct((512, 1024), jnp.bfloat16),
        scratch_shapes=[
            pltpu.VMEM((4096, 128), jnp.float32),
            pltpu.VMEM((4, 512, 256), jnp.bfloat16),
            pltpu.SemaphoreType.DMA((4,)),
        ],
        name="last",
        compiler_params=pltpu.CompilerParams(vmem_limit_bytes=16 << 20),
    )(moved)


def on_device(amplitudes, hop_blocks, coupling_seed):
    sent, rows, base, side = step_one(amplitudes, hop_blocks, coupling_seed)
    sent = exchange(sent, EX1)
    sent = exchange(step_two(sent, rows, base, side), EX2)
    sent = exchange(step_three_four(sent, hop_blocks), EX3)
    return finish(sent)


def solution(mesh):
    fine = Mesh(mesh.devices.reshape(SIZES), AXES)
    spec = P(("z1", "z0", "yh", "y0"), ("zh", "core", "x"))
    return jax.shard_map(
        on_device, mesh=fine, in_specs=(spec, P(), P()), out_specs=spec, check_vma=False
    )
```
